32 devices in a mesh: dp: 1 (over z), sub: 4 (over y), ep: 8 (over x, core).
Axes of the slice: x: 4, y: 4, z: 1, core: 2. Of those that a mesh axis runs over, the one named last changes fastest.
The devices are a block of a 4x4x8 slice.
Arguments:
- input_a: bfloat16 [32, 512, 2048], P(('dp', 'ep', 'sub'))
- input_b: bfloat16 [32, 512, 2048], P(('dp', 'ep', 'sub'))
- route_idx: int32 [2, 16384, 8], P(None, ('dp', 'ep', 'sub'))
- route_gate: float32 [2, 16384, 8], P(None, ('dp', 'ep', 'sub'))
- attn_norm: float32 [2048], replicated
- w_query: bfloat16 [2048, 32, 128], replicated
- w_key: bfloat16 [2048, 32, 128], replicated
- w_value: bfloat16 [2048, 32, 128], replicated
- w_out: bfloat16 [32, 128, 2048], replicated
- moe_norm: float32 [2048], replicated
- w_gate: bfloat16 [128, 2048, 768], P(('ep', 'sub'))
- w_up: bfloat16 [128, 2048, 768], P(('ep', 'sub'))
- w_down: bfloat16 [128, 768, 2048], P(('ep', 'sub'))
Outputs:
- output 1: bfloat16 [32, 512, 2048], P(('dp', 'ep', 'sub'))
- output 2: bfloat16 [32, 512, 2048], P(('dp', 'ep', 'sub'))
All inputs are finite; a program needn't handle non-finite values.
Results may differ from the reference program's by a relative error of at most 0.0126963.
Values are sent between devices in bfloat16 or wider.
A program may use at most 768 MiB of HBM per device.

```python
import functools
import jax
import jax.numpy as jnp
from jax import lax

MODEL_DIM = 2048
NUM_HEADS = 32
HEAD_DIM = 128
FF_DIM = 768
TOP_K = 8
TOK_DEV = 512
SEQ_LEN = 512
EXP_LOCAL = 4
EP_SIZE = 8
SUB_SIZE = 4
NODE_LIM = 4

NUM_DEV = EP_SIZE * SUB_SIZE
NUM_EXP = EXP_LOCAL * NUM_DEV
NUM_TOK = NUM_DEV * TOK_DEV
NUM_SEQ = NUM_TOK // SEQ_LEN
CAP_SLOTS = 3 * TOP_K * TOK_DEV // (2 * NUM_EXP)
EXP_ROOM = NUM_DEV * CAP_SLOTS
NODE_EXP = SUB_SIZE * EXP_LOCAL
PER_VISIT = TOP_K // NODE_LIM
HOT_VISITS = 3 * NODE_LIM * TOK_DEV // (2 * EP_SIZE)
COLD_VISITS = NODE_LIM * TOK_DEV // (2 * EP_SIZE)
NORM_EPS = 1e-6


def draw_device_routes(rng_key):
    key_hot, key_tok, key_exp = jax.random.split(rng_key, 3)
    node_rank = jax.random.permutation(key_hot, jnp.arange(EP_SIZE))
    visits = jnp.where(node_rank < EP_SIZE // 2, HOT_VISITS, COLD_VISITS)
    run_ends = jnp.cumsum(visits)
    run_starts = run_ends - visits
    positions = jnp.arange(NODE_LIM * TOK_DEV)
    node_of = jnp.sum(positions[:, None] >= run_ends[None, :], axis=1)
    within = positions - run_starts[node_of]
    node_visits = visits[node_of]
    copies = node_visits * PER_VISIT // NODE_EXP
    list_pos = jnp.arange(PER_VISIT)[None, :] * node_visits[:, None] + within[:, None]
    local_rank = list_pos // copies[:, None]
    exp_keys = jax.random.split(key_exp, EP_SIZE)
    exp_perm = jax.vmap(jax.random.permutation)(exp_keys, jnp.tile(jnp.arange(NODE_EXP), (EP_SIZE, 1)))
    expert = node_of[:, None] * NODE_EXP + exp_perm[node_of[:, None], local_rank]
    expert = expert.reshape(NODE_LIM, TOK_DEV, PER_VISIT).transpose(1, 0, 2).reshape(TOK_DEV, TOP_K)
    tok_perm = jax.random.permutation(key_tok, jnp.arange(TOK_DEV))
    return expert[tok_perm].astype(jnp.int32)


def setup_inputs(seed: int = 0, part: int = 0) -> dict:
    part_key = jax.random.fold_in(jax.random.key(seed), part)
    part_keys = jax.random.split(part_key, 4)
    tok_shape = (NUM_SEQ, SEQ_LEN, MODEL_DIM)
    input_a = jax.random.normal(part_keys[0], tok_shape, jnp.float32).astype(jnp.bfloat16)
    input_b = jax.random.normal(part_keys[1], tok_shape, jnp.float32).astype(jnp.bfloat16)
    route_keys = jax.random.split(part_keys[2], 2 * NUM_DEV)
    route_idx = jax.vmap(draw_device_routes)(route_keys).reshape(2, NUM_TOK, TOP_K)
    logits = 0.5 * jax.random.normal(part_keys[3], (2, NUM_TOK, TOP_K), jnp.float32)
    route_gate = TOP_K * jax.nn.softmax(logits, axis=-1)
    w_keys = jax.random.split(jax.random.key(seed + 1), 9)
    proj_shape = (MODEL_DIM, NUM_HEADS, HEAD_DIM)
    attn_norm = jax.random.uniform(w_keys[0], (MODEL_DIM,), jnp.float32, 0.5, 1.5)
    w_query = (jax.random.normal(w_keys[1], proj_shape, jnp.float32) * MODEL_DIM ** -0.5).astype(jnp.bfloat16)
    w_key = (jax.random.normal(w_keys[2], proj_shape, jnp.float32) * MODEL_DIM ** -0.5).astype(jnp.bfloat16)
    w_value = (jax.random.normal(w_keys[3], proj_shape, jnp.float32) * MODEL_DIM ** -0.5).astype(jnp.bfloat16)
    w_out = (jax.random.normal(w_keys[4], (NUM_HEADS, HEAD_DIM, MODEL_DIM), jnp.float32) * (2.0 * (NUM_HEADS * HEAD_DIM) ** -0.5)).astype(jnp.bfloat16)
    moe_norm = jax.random.uniform(w_keys[5], (MODEL_DIM,), jnp.float32, 0.5, 1.5)
    w_gate = (jax.random.normal(w_keys[6], (NUM_EXP, MODEL_DIM, FF_DIM), jnp.float32) * MODEL_DIM ** -0.5).astype(jnp.bfloat16)
    w_up = (jax.random.normal(w_keys[7], (NUM_EXP, MODEL_DIM, FF_DIM), jnp.float32) * MODEL_DIM ** -0.5).astype(jnp.bfloat16)
    w_down = (jax.random.normal(w_keys[8], (NUM_EXP, FF_DIM, MODEL_DIM), jnp.float32) * FF_DIM ** -0.5).astype(jnp.bfloat16)
    return {'input_a': input_a, 'input_b': input_b, 'route_idx': route_idx, 'route_gate': route_gate, 'attn_norm': attn_norm, 'w_query': w_query, 'w_key': w_key, 'w_value': w_value, 'w_out': w_out, 'moe_norm': moe_norm, 'w_gate': w_gate, 'w_up': w_up, 'w_down': w_down}


def rms_norm(values, norm_gain):
    acc_f32 = values.astype(jnp.float32)
    inv_rms = lax.rsqrt(jnp.mean(acc_f32 * acc_f32, axis=-1, keepdims=True) + NORM_EPS)
    return (acc_f32 * inv_rms * norm_gain).astype(jnp.bfloat16)


def attention_seq(seq_tok, attn_norm, w_query, w_key, w_value, w_out):
    normed = rms_norm(seq_tok, attn_norm).astype(jnp.float32)
    q_heads = jnp.einsum('sd,dhc->shc', normed, w_query.astype(jnp.float32)).astype(jnp.bfloat16)
    k_heads = jnp.einsum('sd,dhc->shc', normed, w_key.astype(jnp.float32)).astype(jnp.bfloat16)
    v_heads = jnp.einsum('sd,dhc->shc', normed, w_value.astype(jnp.float32)).astype(jnp.bfloat16)
    scores = jnp.einsum('qhc,khc->hqk', q_heads.astype(jnp.float32), k_heads.astype(jnp.float32)) * HEAD_DIM ** -0.5
    causal = jnp.arange(SEQ_LEN)[:, None] >= jnp.arange(SEQ_LEN)[None, :]
    scores = jnp.where(causal[None, :, :], scores, -jnp.inf)
    prob_bf = jax.nn.softmax(scores, axis=-1).astype(jnp.bfloat16)
    context = jnp.einsum('hqk,khc->qhc', prob_bf.astype(jnp.float32), v_heads.astype(jnp.float32)).astype(jnp.bfloat16)
    proj_out = jnp.einsum('qhc,hcd->qd', context.astype(jnp.float32), w_out.astype(jnp.float32))
    return (seq_tok.astype(jnp.float32) + proj_out).astype(jnp.bfloat16)


def expert_apply(operands):
    expert_rows, gate_mat, up_mat, down_mat = operands
    gate_h = jnp.dot(expert_rows, gate_mat, preferred_element_type=jnp.float32)
    up_h = jnp.dot(expert_rows, up_mat, preferred_element_type=jnp.float32)
    act_rows = (jax.nn.silu(gate_h) * up_h).astype(jnp.bfloat16)
    return jnp.dot(act_rows, down_mat, preferred_element_type=jnp.float32).astype(jnp.bfloat16)


def moe_layer(hidden, exp_ids, gate_w, moe_norm, w_gate, w_up, w_down):
    normed = rms_norm(hidden, moe_norm)
    flat_ids = exp_ids.reshape(-1)
    sort_order = jnp.argsort(flat_ids, stable=True)
    sorted_ids = flat_ids[sort_order]
    counts = jnp.bincount(flat_ids, length=NUM_EXP)
    starts = jnp.cumsum(counts) - counts
    slot_rank = jnp.arange(NUM_TOK * TOP_K) - starts[sorted_ids]
    slot_sorted = sorted_ids * EXP_ROOM + slot_rank
    holder = jnp.full((NUM_EXP * EXP_ROOM,), NUM_TOK, jnp.int32).at[slot_sorted].set(sort_order // TOP_K)
    disp_rows = jnp.take(normed, holder, axis=0, mode='fill', fill_value=0).reshape(NUM_EXP, EXP_ROOM, MODEL_DIM)
    expert_out = lax.map(expert_apply, (disp_rows, w_gate, w_up, w_down))
    slot_of = jnp.zeros_like(flat_ids).at[sort_order].set(slot_sorted)
    picked = jnp.take(expert_out.reshape(NUM_EXP * EXP_ROOM, MODEL_DIM), slot_of, axis=0).reshape(NUM_TOK, TOP_K, MODEL_DIM)
    moe_sum = jnp.sum(gate_w[:, :, None] * picked.astype(jnp.float32), axis=1)
    return (hidden.astype(jnp.float32) + moe_sum).astype(jnp.bfloat16)


def reference(input_a, input_b, route_idx, route_gate, attn_norm, w_query, w_key, w_value, w_out, moe_norm, w_gate, w_up, w_down):
    attend = functools.partial(attention_seq, attn_norm=attn_norm, w_query=w_query, w_key=w_key, w_value=w_value, w_out=w_out)

    def micro_pass(tokens, exp_ids, gate_w):
        hidden = lax.map(attend, tokens).reshape(NUM_TOK, MODEL_DIM)
        mixed_out = moe_layer(hidden, exp_ids, gate_w, moe_norm, w_gate, w_up, w_down)
        return mixed_out.reshape(NUM_SEQ, SEQ_LEN, MODEL_DIM)

    return micro_pass(input_a, route_idx[0], route_gate[0]), micro_pass(input_b, route_idx[1], route_gate[1])
```

```python
import functools

import jax
import jax.numpy as jnp
from jax import lax
from jax.experimental import pallas as pl
from jax.experimental.pallas import tpu as pltpu
from jax.sharding import PartitionSpec as P

NORM_EPS = 1e-6
VMEM_MAX = 60 * 1024 * 1024
F32 = jnp.float32
BF16 = jnp.bfloat16


def rms_norm(values, norm_gain):
    acc_f32 = values.astype(F32)
    inv_rms = lax.rsqrt(jnp.mean(acc_f32 * acc_f32, axis=-1, keepdims=True) + NORM_EPS)
    return (acc_f32 * inv_rms * norm_gain).astype(BF16)


def attn_kernel(scale, q_ref, k_ref, v_ref, o_ref):
    heads, seq_len, head_dim = q_ref.shape
    half = seq_len // 2
    for h in range(heads):
        for part in range(2):
            keys = (part + 1) * half
            q = q_ref[h, part * half:keys, :]
            k = k_ref[h, :keys, :]
            s = lax.dot_general(q, k, (((1,), (1,)), ((), ())), preferred_element_type=F32) * scale
            rows = lax.broadcasted_iota(jnp.int32, s.shape, 0) + part * half
            cols = lax.broadcasted_iota(jnp.int32, s.shape, 1)
            s = jnp.where(rows >= cols, s, -jnp.inf)
            p = jnp.exp(s - jnp.max(s, axis=-1, keepdims=True))
            p = (p / jnp.sum(p, axis=-1, keepdims=True)).astype(BF16)
            o = jnp.dot(p, v_ref[h, :keys, :], preferred_element_type=F32)
            o_ref[part * half:keys, h * head_dim:(h + 1) * head_dim] = o.astype(BF16)


def attention_core(q, k, v):
    heads, seq_len, head_dim = q.shape
    step = 4
    spec = pl.BlockSpec((step, seq_len, head_dim), lambda i: (i, 0, 0))
    return pl.pallas_call(
        functools.partial(attn_kernel, head_dim ** -0.5),
        grid=(heads // step,),
        out_shape=jax.ShapeDtypeStruct((seq_len, heads * head_dim), BF16),
        in_specs=[spec, spec, spec],
        out_specs=pl.BlockSpec((seq_len, step * head_dim), lambda i: (0, i)),
        cost_estimate=pl.CostEstimate(flops=4 * heads * seq_len * seq_len * head_dim, bytes_accessed=8 * heads * seq_len * head_dim, transcendentals=heads * seq_len * seq_len),
        name="attention_core",
    )(q, k, v)


def attention_block(seq, attn_norm, w_query, w_key, w_value, w_out):
    normed = rms_norm(seq, attn_norm)
    q, k, v = (jnp.einsum('sd,dhc->hsc', normed, w, preferred_element_type=F32).astype(BF16) for w in (w_query, w_key, w_value))
    context = attention_core(q, k, v)
    w_flat = w_out.reshape(-1, w_out.shape[-1])
    proj_out = jnp.dot(context, w_flat, preferred_element_type=F32)
    return (seq.astype(F32) + proj_out).astype(BF16)


def pick_kernel(slot_ref, rows_ref, out_ref):
    exp_local, _, cap, _ = out_ref.shape
    toks = rows_ref.shape[1]
    want = lax.broadcasted_iota(jnp.int32, (cap, toks), 0)
    for e in range(exp_local):
        sel = (want == slot_ref[0, e:e + 1, :]).astype(F32).astype(BF16)
        out_ref[e, 0] = jnp.dot(sel, rows_ref[0], preferred_element_type=F32).astype(BF16)


def pick_rows(slots, rows, cap):
    srcs, exps, toks = slots.shape
    dim = rows.shape[-1]
    return pl.pallas_call(
        pick_kernel,
        grid=(srcs,),
        out_shape=jax.ShapeDtypeStruct((exps, srcs, cap, dim), BF16),
        in_specs=[pl.BlockSpec((1, exps, toks), lambda s: (s, 0, 0)), pl.BlockSpec((1, toks, dim), lambda s: (s, 0, 0))],
        out_specs=pl.BlockSpec((exps, 1, cap, dim), lambda s: (0, s, 0, 0)),
        cost_estimate=pl.CostEstimate(flops=2 * srcs * exps * cap * toks * dim, bytes_accessed=2 * srcs * (toks + exps * cap) * dim, transcendentals=0),
        name="pick_rows",
    )(slots, rows)


def ffn_kernel(x_ref, wg_ref, wu_ref, wd_ref, o_ref):
    _, srcs, cap, dim = x_ref.shape
    x = x_ref[0].reshape(srcs * cap, dim)
    gate_h = jnp.dot(x, wg_ref[0], preferred_element_type=F32)
    up_h = jnp.dot(x, wu_ref[0], preferred_element_type=F32)
    act = (jax.nn.silu(gate_h) * up_h).astype(BF16)
    y = jnp.dot(act, wd_ref[0], preferred_element_type=F32).astype(BF16)
    o_ref[:, 0] = y.reshape(srcs, cap, dim)


def expert_ffn(x, w_gate, w_up, w_down):
    exps, srcs, cap, dim = x.shape
    ff = w_gate.shape[-1]
    step = 8
    return pl.pallas_call(
        ffn_kernel,
        grid=(exps, srcs // step),
        out_shape=jax.ShapeDtypeStruct((srcs, exps, cap, dim), BF16),
        in_specs=[
            pl.BlockSpec((1, step, cap, dim), lambda e, s: (e, s, 0, 0)),
            pl.BlockSpec((1, dim, ff), lambda e, s: (e, 0, 0)),
            pl.BlockSpec((1, dim, ff), lambda e, s: (e, 0, 0)),
            pl.BlockSpec((1, ff, dim), lambda e, s: (e, 0, 0)),
        ],
        out_specs=pl.BlockSpec((step, 1, cap, dim), lambda e, s: (s, e, 0, 0)),
        cost_estimate=pl.CostEstimate(flops=6 * exps * srcs * cap * dim * ff, bytes_accessed=4 * exps * srcs * cap * dim + 6 * exps * dim * ff, transcendentals=exps * srcs * cap * ff),
        compiler_params=pltpu.CompilerParams(vmem_limit_bytes=VMEM_MAX),
        name="expert_ffn",
    )(x, w_gate, w_up, w_down)


def split3(x):
    hi = x.astype(BF16)
    rest = x - hi.astype(F32)
    mid = rest.astype(BF16)
    low = (rest - mid.astype(F32)).astype(BF16)
    return hi, mid, low


def ranks_of(mask, axis):
    toks = mask.shape[axis]
    row = lax.broadcasted_iota(jnp.int32, (toks, toks), 0)
    col = lax.broadcasted_iota(jnp.int32, (toks, toks), 1)
    if axis == mask.ndim - 1:
        tri = (row < col).astype(BF16)
        return jnp.dot(mask.astype(BF16), tri, preferred_element_type=F32).astype(jnp.int32)
    tri = (row > col).astype(BF16)
    return jnp.dot(tri, mask.astype(BF16), preferred_element_type=F32).astype(jnp.int32)


def slots_here(ids_all, first_exp, exp_local):
    mine = first_exp + jnp.arange(exp_local, dtype=jnp.int32)
    mask = jnp.any(ids_all[:, None] == mine[None, :, None, None], axis=2)
    srcs, exps, toks = mask.shape
    rank = ranks_of(mask.reshape(srcs * exps, toks), 1).reshape(srcs, exps, toks)
    return jnp.where(mask, rank, -1)


def home_select(ids, gates, num_exp, cap):
    hit = ids[:, :, None] == jnp.arange(num_exp, dtype=jnp.int32)[None, None, :]
    mask = jnp.any(hit, axis=1)
    gate = jnp.sum(jnp.where(hit, gates[:, :, None], 0.0), axis=1)
    rank = jnp.where(mask, ranks_of(mask, 0), -1)
    here = rank[:, :, None] == jnp.arange(cap, dtype=jnp.int32)[None, None, :]
    parts = [jnp.where(here, g.astype(F32)[:, :, None], 0.0).astype(BF16).reshape(ids.shape[0], num_exp * cap) for g in split3(gate)]
    return jnp.concatenate(parts, axis=0)


def solution(mesh):
    ep_size = mesh.shape['ep']
    sub_size = mesh.shape['sub']
    axes = ('ep', 'sub')
    tok_spec = P(('dp', 'ep', 'sub'), None, None)
    route_spec = P(None, ('dp', 'ep', 'sub'), None)
    exp_spec = P(('ep', 'sub'), None, None)

    def device_body(input_a, input_b, route_idx, route_gate, attn_norm, w_query, w_key, w_value, w_out, moe_norm, w_gate, w_up, w_down):
        exp_local = w_gate.shape[0]
        num_dev = ep_size * sub_size
        num_exp = exp_local * num_dev
        tok_count, top_k = route_idx.shape[1:]
        model_dim = input_a.shape[-1]
        cap = 3 * top_k * tok_count // (2 * num_exp)
        first_exp = lax.axis_index(axes) * exp_local

        ids_all = lax.all_gather(jnp.swapaxes(route_idx, 1, 2), axes, axis=0)

        hiddens, gathered = [], []
        for tokens in (input_a, input_b):
            hidden = attention_block(tokens.reshape(tok_count, model_dim), attn_norm, w_query, w_key, w_value, w_out)
            normed = rms_norm(hidden, moe_norm)
            gathered.append(lax.all_gather(normed, axes, axis=0))
            hiddens.append(hidden)

        outs = []
        for mb, tokens in enumerate((input_a, input_b)):
            slots = slots_here(ids_all[:, mb], first_exp, exp_local)
            picked = pick_rows(slots, gathered[mb], cap)
            expert_out = expert_ffn(picked, w_gate, w_up, w_down)
            returned = lax.all_to_all(expert_out, axes, 0, 0, tiled=True).reshape(num_exp * cap, model_dim)
            select = home_select(route_idx[mb], route_gate[mb], num_exp, cap)
            sums = jnp.dot(select, returned, preferred_element_type=F32).reshape(3, tok_count, model_dim)
            moe_sum = sums[0] + (sums[1] + sums[2])
            outs.append((hiddens[mb].astype(F32) + moe_sum).astype(BF16).reshape(tokens.shape))
        return outs[0], outs[1]

    return jax.shard_map(device_body, mesh=mesh, in_specs=(tok_spec, tok_spec, route_spec, route_spec, P(), P(), P(), P(), P(), P(), exp_spec, exp_spec, exp_spec), out_specs=(tok_spec, tok_spec), check_vma=False)
```

```python
import functools

import jax
import jax.numpy as jnp
from jax import lax
from jax.experimental import pallas as pl
from jax.experimental.pallas import tpu as pltpu
from jax.sharding import PartitionSpec as P

NORM_EPS = 1e-6
VMEM_MAX = 60 * 1024 * 1024
F32 = jnp.float32
BF16 = jnp.bfloat16


def rms_norm(values, norm_gain):
    acc_f32 = values.astype(F32)
    inv_rms = lax.rsqrt(jnp.mean(acc_f32 * acc_f32, axis=-1, keepdims=True) + NORM_EPS)
    return (acc_f32 * inv_rms * norm_gain).astype(BF16)


def attn_kernel(scale, first, q_ref, *refs):
    k_refs, v_refs, o_ref = refs[:first + 1], refs[first + 1:2 * first + 2], refs[-1]
    heads, q_len, head_dim = q_ref.shape
    parts = 2 if first == 0 and q_len >= 512 else 1
    rows_per = q_len // parts
    for h in range(heads):
        for part in range(parts):
            q = q_ref[h, part * rows_per:(part + 1) * rows_per, :]
            spans = [(k_refs[i], v_refs[i], 0, k_refs[i].shape[1], False) for i in range(first)]
            if part:
                spans.append((k_refs[first], v_refs[first], 0, part * rows_per, False))
            spans.append((k_refs[first], v_refs[first], part * rows_per, (part + 1) * rows_per, True))
            scores = []
            for k_ref, _, lo, hi, diagonal in spans:
                s = lax.dot_general(q, k_ref[h, lo:hi, :], (((1,), (1,)), ((), ())), preferred_element_type=F32) * scale
                if diagonal:
                    rows = lax.broadcasted_iota(jnp.int32, s.shape, 0)
                    cols = lax.broadcasted_iota(jnp.int32, s.shape, 1)
                    s = jnp.where(rows >= cols, s, -jnp.inf)
                scores.append(s)
            top = functools.reduce(jnp.maximum, [jnp.max(s, axis=-1, keepdims=True) for s in scores])
            probs = [jnp.exp(s - top) for s in scores]
            inv = 1.0 / functools.reduce(jnp.add, [jnp.sum(p, axis=-1, keepdims=True) for p in probs])
            o = None
            for p, (_, v_ref, lo, hi, _) in zip(probs, spans):
                term = jnp.dot((p * inv).astype(BF16), v_ref[h, lo:hi, :], preferred_element_type=F32)
                o = term if o is None else o + term
            o_ref[part * rows_per:(part + 1) * rows_per, h * head_dim:(h + 1) * head_dim] = o.astype(BF16)


def attention_core(q, ks, vs):
    heads, q_len, head_dim = q.shape
    step = 4
    spec = lambda t: pl.BlockSpec((step, t.shape[1], head_dim), lambda i: (i, 0, 0))
    keys = sum(k.shape[1] for k in ks)
    return pl.pallas_call(
        functools.partial(attn_kernel, head_dim ** -0.5, len(ks) - 1),
        grid=(heads // step,),
        out_shape=jax.ShapeDtypeStruct((q_len, heads * head_dim), BF16),
        in_specs=[spec(t) for t in (q, *ks, *vs)],
        out_specs=pl.BlockSpec((q_len, step * head_dim), lambda i: (0, i)),
        cost_estimate=pl.CostEstimate(flops=4 * heads * q_len * keys * head_dim, bytes_accessed=4 * heads * (q_len + keys) * head_dim, transcendentals=heads * q_len * keys),
        name="attention_core",
    )(q, *ks, *vs)


def attention_rows(rows, ks, vs, attn_norm, w_query, w_key, w_value, w_out):
    normed = rms_norm(rows, attn_norm)
    q, k, v = (jnp.einsum('sd,dhc->hsc', normed, w, preferred_element_type=F32).astype(BF16) for w in (w_query, w_key, w_value))
    ks, vs = ks + [k], vs + [v]
    context = attention_core(q, ks, vs)
    proj_out = jnp.dot(context, w_out.reshape(-1, w_out.shape[-1]), preferred_element_type=F32)
    return (rows.astype(F32) + proj_out).astype(BF16), ks, vs


def pick_kernel(slot_ref, *refs):
    row_refs, out_ref = refs[:-1], refs[-1]
    exp_local, _, cap, dim = out_ref.shape
    total = None
    lo = 0
    for rows_ref in row_refs:
        toks = rows_ref.shape[1]
        want = lax.broadcasted_iota(jnp.int32, (cap, toks), 0)
        sel = jnp.concatenate([(want == slot_ref[0, e:e + 1, lo:lo + toks]).astype(F32) for e in range(exp_local)], axis=0).astype(BF16)
        term = jnp.dot(sel, rows_ref[0], preferred_element_type=F32)
        total = term if total is None else total + term
        lo += toks
    out_ref[:, 0] = total.astype(BF16).reshape(exp_local, cap, dim)


def pick_rows(slots, ranges, cap):
    srcs, exps, toks = slots.shape
    dim = ranges[0].shape[-1]
    return pl.pallas_call(
        pick_kernel,
        grid=(srcs,),
        out_shape=jax.ShapeDtypeStruct((exps, srcs, cap, dim), BF16),
        in_specs=[pl.BlockSpec((1, exps, toks), lambda s: (s, 0, 0))] + [pl.BlockSpec((1, r.shape[1], dim), lambda s: (s, 0, 0)) for r in ranges],
        out_specs=pl.BlockSpec((exps, 1, cap, dim), lambda s: (0, s, 0, 0)),
        cost_estimate=pl.CostEstimate(flops=2 * srcs * exps * cap * toks * dim, bytes_accessed=2 * srcs * (toks + exps * cap) * dim, transcendentals=0),
        name="pick_rows",
    )(slots, *ranges)


def ffn_kernel(x_ref, wg_ref, wu_ref, wd_ref, *o_refs):
    _, srcs, cap, dim = x_ref.shape
    x = x_ref[0].reshape(srcs * cap, dim)
    gate_h = jnp.dot(x, wg_ref[0], preferred_element_type=F32)
    up_h = jnp.dot(x, wu_ref[0], preferred_element_type=F32)
    act = (jax.nn.silu(gate_h) * up_h).astype(BF16)
    y = jnp.dot(act, wd_ref[0], preferred_element_type=F32).astype(BF16)
    lo = 0
    for o_ref in o_refs:
        width = o_ref.shape[-1]
        o_ref[:, 0] = y[:, lo:lo + width].reshape(srcs, cap, width)
        lo += width


def expert_ffn(x, w_gate, w_up, w_down, pieces):
    exps, srcs, cap, dim = x.shape
    ff = w_gate.shape[-1]
    step = 8
    width = dim // pieces
    return pl.pallas_call(
        ffn_kernel,
        grid=(exps, srcs // step),
        out_shape=[jax.ShapeDtypeStruct((srcs, exps, cap, width), BF16)] * pieces,
        in_specs=[
            pl.BlockSpec((1, step, cap, dim), lambda e, s: (e, s, 0, 0)),
            pl.BlockSpec((1, dim, ff), lambda e, s: (e, 0, 0)),
            pl.BlockSpec((1, dim, ff), lambda e, s: (e, 0, 0)),
            pl.BlockSpec((1, ff, dim), lambda e, s: (e, 0, 0)),
        ],
        out_specs=[pl.BlockSpec((step, 1, cap, width), lambda e, s: (s, e, 0, 0))] * pieces,
        cost_estimate=pl.CostEstimate(flops=6 * exps * srcs * cap * dim * ff, bytes_accessed=4 * exps * srcs * cap * dim + 6 * exps * dim * ff, transcendentals=exps * srcs * cap * ff),
        compiler_params=pltpu.CompilerParams(vmem_limit_bytes=VMEM_MAX),
        name="expert_ffn",
    )(x, w_gate, w_up, w_down)


def split3(x):
    hi = x.astype(BF16)
    rest = x - hi.astype(F32)
    mid = rest.astype(BF16)
    low = (rest - mid.astype(F32)).astype(BF16)
    return hi, mid, low


def ranks_of(mask, axis):
    toks = mask.shape[axis]
    row = lax.broadcasted_iota(jnp.int32, (toks, toks), 0)
    col = lax.broadcasted_iota(jnp.int32, (toks, toks), 1)
    if axis == mask.ndim - 1:
        tri = (row < col).astype(BF16)
        return jnp.dot(mask.astype(BF16), tri, preferred_element_type=F32).astype(jnp.int32)
    tri = (row > col).astype(BF16)
    return jnp.dot(tri, mask.astype(BF16), preferred_element_type=F32).astype(jnp.int32)


def slots_here(ids_all, first_exp, exp_local):
    mine = first_exp + jnp.arange(exp_local, dtype=jnp.int32)
    mask = jnp.any(ids_all[:, None] == mine[None, :, None, None], axis=2)
    srcs, exps, toks = mask.shape
    rank = ranks_of(mask.reshape(srcs * exps, toks), 1).reshape(srcs, exps, toks)
    return jnp.where(mask, rank, -1)


def home_select(ids, gates, num_exp, cap):
    hit = ids[:, :, None] == jnp.arange(num_exp, dtype=jnp.int32)[None, None, :]
    mask = jnp.any(hit, axis=1)
    gate = jnp.sum(jnp.where(hit, gates[:, :, None], 0.0), axis=1)
    rank = jnp.where(mask, ranks_of(mask, 0), -1)
    here = rank[:, :, None] == jnp.arange(cap, dtype=jnp.int32)[None, None, :]
    parts = [jnp.where(here, g.astype(F32)[:, :, None], 0.0).astype(BF16).reshape(ids.shape[0], num_exp * cap) for g in split3(gate)]
    return jnp.concatenate(parts, axis=0)


def solution(mesh):
    ep_size = mesh.shape['ep']
    sub_size = mesh.shape['sub']
    axes = ('ep', 'sub')
    tok_spec = P(('dp', 'ep', 'sub'), None, None)
    route_spec = P(None, ('dp', 'ep', 'sub'), None)
    exp_spec = P(('ep', 'sub'), None, None)

    def device_body(input_a, input_b, route_idx, route_gate, attn_norm, w_query, w_key, w_value, w_out, moe_norm, w_gate, w_up, w_down):
        exp_local = w_gate.shape[0]
        num_dev = ep_size * sub_size
        num_exp = exp_local * num_dev
        tok_count, top_k = route_idx.shape[1:]
        model_dim = input_a.shape[-1]
        cap = 3 * top_k * tok_count // (2 * num_exp)
        first_exp = lax.axis_index(axes) * exp_local

        ids_all = lax.all_gather(jnp.swapaxes(route_idx, 1, 2), axes, axis=0)

        weights = (attn_norm, w_query, w_key, w_value, w_out)
        hiddens, gathered = [], []
        after = None
        for tokens, ranges in ((input_a, 2), (input_b, 1)):
            rows_all = tokens.reshape(tok_count, model_dim)
            step = tok_count // ranges
            ks, vs, parts, blocks = [], [], [], []
            for r in range(ranges):
                rows = rows_all[r * step:(r + 1) * step]
                if after is not None:
                    rows, after = lax.optimization_barrier((rows, after))
                hidden, ks, vs = attention_rows(rows, ks, vs, *weights)
                after = rms_norm(hidden, moe_norm)
                blocks.append(lax.all_gather(after, axes, axis=0))
                parts.append(hidden)
            hiddens.append(jnp.concatenate(parts, axis=0) if ranges > 1 else parts[0])
            gathered.append(blocks)

        expert_outs = []
        for mb, pieces in ((0, 1), (1, 1)):
            slots = slots_here(ids_all[:, mb], first_exp, exp_local)
            picked = pick_rows(slots, gathered[mb], cap)
            expert_outs.append(expert_ffn(picked, w_gate, w_up, w_down, pieces))
            if mb == 0:
                expert_outs[0], gathered[1] = lax.optimization_barrier((expert_outs[0], gathered[1]))

        outs = []
        for mb, tokens in enumerate((input_a, input_b)):
            select = home_select(route_idx[mb], route_gate[mb], num_exp, cap)
            pieces = []
            lo = 0
            for piece in expert_outs[mb]:
                width = piece.shape[-1]
                returned = lax.all_to_all(piece, axes, 0, 0, tiled=True).reshape(num_exp * cap, width)
                sums = jnp.dot(select, returned, preferred_element_type=F32).reshape(3, tok_count, width)
                moe_sum = sums[0] + (sums[1] + sums[2])
                pieces.append((hiddens[mb][:, lo:lo + width].astype(F32) + moe_sum).astype(BF16))
                lo += width
            outs.append((jnp.concatenate(pieces, axis=1) if len(pieces) > 1 else pieces[0]).reshape(tokens.shape))
        return outs[0], outs[1]

    return jax.shard_map(device_body, mesh=mesh, in_specs=(tok_spec, tok_spec, route_spec, route_spec, P(), P(), P(), P(), P(), P(), exp_spec, exp_spec, exp_spec), out_specs=(tok_spec, tok_spec), check_vma=False)
```

```python
import functools

import jax
import jax.numpy as jnp
from jax import lax
from jax.experimental import pallas as pl
from jax.experimental.pallas import tpu as pltpu
from jax.sharding import PartitionSpec as P

NORM_EPS = 1e-6
VMEM_MAX = 60 * 1024 * 1024
F32 = jnp.float32
BF16 = jnp.bfloat16
MESH = pl.DeviceIdType.MESH
CORES = 2


def rms_norm(values, norm_gain):
    acc_f32 = values.astype(F32)
    inv_rms = lax.rsqrt(jnp.mean(acc_f32 * acc_f32, axis=-1, keepdims=True) + NORM_EPS)
    return (acc_f32 * inv_rms * norm_gain).astype(BF16)


def attn_kernel(scale, first, q_ref, *refs):
    k_refs, v_refs, o_ref = refs[:first + 1], refs[first + 1:2 * first + 2], refs[-1]
    heads, q_len, head_dim = q_ref.shape
    parts = 2 if first == 0 and q_len >= 512 else 1
    rows_per = q_len // parts
    for h in range(heads):
        for part in range(parts):
            q = q_ref[h, part * rows_per:(part + 1) * rows_per, :]
            spans = [(k_refs[i], v_refs[i], 0, k_refs[i].shape[1], False) for i in range(first)]
            if part:
                spans.append((k_refs[first], v_refs[first], 0, part * rows_per, False))
            spans.append((k_refs[first], v_refs[first], part * rows_per, (part + 1) * rows_per, True))
            scores = []
            for k_ref, _, lo, hi, diagonal in spans:
                s = lax.dot_general(q, k_ref[h, lo:hi, :], (((1,), (1,)), ((), ())), preferred_element_type=F32) * scale
                if diagonal:
                    rows = lax.broadcasted_iota(jnp.int32, s.shape, 0)
                    cols = lax.broadcasted_iota(jnp.int32, s.shape, 1)
                    s = jnp.where(rows >= cols, s, -jnp.inf)
                scores.append(s)
            top = functools.reduce(jnp.maximum, [jnp.max(s, axis=-1, keepdims=True) for s in scores])
            probs = [jnp.exp(s - top) for s in scores]
            inv = 1.0 / functools.reduce(jnp.add, [jnp.sum(p, axis=-1, keepdims=True) for p in probs])
            o = None
            for p, (_, v_ref, lo, hi, _) in zip(probs, spans):
                term = jnp.dot((p * inv).astype(BF16), v_ref[h, lo:hi, :], preferred_element_type=F32)
                o = term if o is None else o + term
            o_ref[part * rows_per:(part + 1) * rows_per, h * head_dim:(h + 1) * head_dim] = o.astype(BF16)


def attention_core(q, ks, vs):
    heads, q_len, head_dim = q.shape
    step = 4
    spec = lambda t: pl.BlockSpec((step, t.shape[1], head_dim), lambda i: (i, 0, 0))
    keys = sum(k.shape[1] for k in ks)
    return pl.pallas_call(
        functools.partial(attn_kernel, head_dim ** -0.5, len(ks) - 1),
        grid=(heads // step,),
        out_shape=jax.ShapeDtypeStruct((q_len, heads * head_dim), BF16),
        in_specs=[spec(t) for t in (q, *ks, *vs)],
        out_specs=pl.BlockSpec((q_len, step * head_dim), lambda i: (0, i)),
        cost_estimate=pl.CostEstimate(flops=4 * heads * q_len * keys * head_dim, bytes_accessed=4 * heads * (q_len + keys) * head_dim, transcendentals=heads * q_len * keys),
        name="attention_core",
    )(q, *ks, *vs)


def attention_rows(rows, ks, vs, attn_norm, w_query, w_key, w_value, w_out):
    normed = rms_norm(rows, attn_norm)
    q, k, v = (jnp.einsum('sd,dhc->hsc', normed, w, preferred_element_type=F32).astype(BF16) for w in (w_query, w_key, w_value))
    ks, vs = ks + [k], vs + [v]
    context = attention_core(q, ks, vs)
    proj_out = jnp.dot(context, w_out.reshape(-1, w_out.shape[-1]), preferred_element_type=F32)
    return (rows.astype(F32) + proj_out).astype(BF16), ks, vs


def pick_kernel(slot_ref, *refs):
    row_refs, out_ref = refs[:-1], refs[-1]
    exp_local, _, cap, dim = out_ref.shape
    total = None
    lo = 0
    for rows_ref in row_refs:
        toks = rows_ref.shape[1]
        want = lax.broadcasted_iota(jnp.int32, (cap, toks), 0)
        sel = jnp.concatenate([(want == slot_ref[0, e:e + 1, lo:lo + toks]).astype(F32) for e in range(exp_local)], axis=0).astype(BF16)
        term = jnp.dot(sel, rows_ref[0], preferred_element_type=F32)
        total = term if total is None else total + term
        lo += toks
    out_ref[:, 0] = total.astype(BF16).reshape(exp_local, cap, dim)


def pick_rows(slots, ranges, cap):
    srcs, exps, toks = slots.shape
    dim = ranges[0].shape[-1]
    return pl.pallas_call(
        pick_kernel,
        grid=(srcs,),
        out_shape=jax.ShapeDtypeStruct((exps, srcs, cap, dim), BF16),
        in_specs=[pl.BlockSpec((1, exps, toks), lambda s: (s, 0, 0))] + [pl.BlockSpec((1, r.shape[1], dim), lambda s: (s, 0, 0)) for r in ranges],
        out_specs=pl.BlockSpec((exps, 1, cap, dim), lambda s: (0, s, 0, 0)),
        cost_estimate=pl.CostEstimate(flops=2 * srcs * exps * cap * toks * dim, bytes_accessed=2 * srcs * (toks + exps * cap) * dim, transcendentals=0),
        name="pick_rows",
    )(slots, *ranges)


def ffn_kernel(x_ref, wg_ref, wu_ref, wd_ref, *o_refs):
    _, srcs, cap, dim = x_ref.shape
    x = x_ref[0].reshape(srcs * cap, dim)
    gate_h = jnp.dot(x, wg_ref[0], preferred_element_type=F32)
    up_h = jnp.dot(x, wu_ref[0], preferred_element_type=F32)
    act = (jax.nn.silu(gate_h) * up_h).astype(BF16)
    y = jnp.dot(act, wd_ref[0], preferred_element_type=F32).astype(BF16)
    lo = 0
    for o_ref in o_refs:
        width = o_ref.shape[-1]
        o_ref[:, 0] = y[:, lo:lo + width].reshape(srcs, cap, width)
        lo += width


def expert_ffn(x, w_gate, w_up, w_down, pieces):
    exps, srcs, cap, dim = x.shape
    ff = w_gate.shape[-1]
    step = 8
    width = dim // pieces
    return pl.pallas_call(
        ffn_kernel,
        grid=(exps, srcs // step),
        out_shape=[jax.ShapeDtypeStruct((srcs, exps, cap, width), BF16)] * pieces,
        in_specs=[
            pl.BlockSpec((1, step, cap, dim), lambda e, s: (e, s, 0, 0)),
            pl.BlockSpec((1, dim, ff), lambda e, s: (e, 0, 0)),
            pl.BlockSpec((1, dim, ff), lambda e, s: (e, 0, 0)),
            pl.BlockSpec((1, ff, dim), lambda e, s: (e, 0, 0)),
        ],
        out_specs=[pl.BlockSpec((step, 1, cap, width), lambda e, s: (s, e, 0, 0))] * pieces,
        cost_estimate=pl.CostEstimate(flops=6 * exps * srcs * cap * dim * ff, bytes_accessed=4 * exps * srcs * cap * dim + 6 * exps * dim * ff, transcendentals=exps * srcs * cap * ff),
        compiler_params=pltpu.CompilerParams(vmem_limit_bytes=VMEM_MAX),
        name="expert_ffn",
    )(x, w_gate, w_up, w_down)


def split3(x):
    hi = x.astype(BF16)
    rest = x - hi.astype(F32)
    mid = rest.astype(BF16)
    low = (rest - mid.astype(F32)).astype(BF16)
    return hi, mid, low


def ranks_of(mask, axis):
    toks = mask.shape[axis]
    row = lax.broadcasted_iota(jnp.int32, (toks, toks), 0)
    col = lax.broadcasted_iota(jnp.int32, (toks, toks), 1)
    if axis == mask.ndim - 1:
        tri = (row < col).astype(BF16)
        return jnp.dot(mask.astype(BF16), tri, preferred_element_type=F32).astype(jnp.int32)
    tri = (row > col).astype(BF16)
    return jnp.dot(tri, mask.astype(BF16), preferred_element_type=F32).astype(jnp.int32)


def slots_here(ids_all, first_exp, exp_local):
    mine = first_exp + jnp.arange(exp_local, dtype=jnp.int32)
    mask = jnp.any(ids_all[:, None] == mine[None, :, None, None], axis=2)
    srcs, exps, toks = mask.shape
    rank = ranks_of(mask.reshape(srcs * exps, toks), 1).reshape(srcs, exps, toks)
    return jnp.where(mask, rank, -1)


def sources_select(ids, gates, experts):
    hit = ids[:, None] == experts[None, :, None, None]
    mask = jnp.any(hit, axis=2)
    gate = jnp.sum(jnp.where(hit, gates[:, None], 0.0), axis=2)
    srcs, exps, toks = mask.shape
    rank = ranks_of(mask.reshape(srcs * exps, toks), 1).reshape(srcs, exps, toks)
    return jnp.where(mask, rank, -1), gate


def place():
    ep = lax.axis_index('ep')
    return lax.div(ep, CORES), lax.rem(ep, CORES), lax.axis_index('sub')


def exchange_copies(el, er, rl, rr, send, recv, own):
    nx, _, ny = el.shape[:3]
    x, c, y = place()
    copies = []
    for dc in range(CORES):
        for dy in range(ny):
            if dc or dy:
                c2, y2, n = lax.rem(c + dc, CORES), lax.rem(y + dy, ny), len(copies)
                copies.append(pltpu.make_async_remote_copy(
                    src_ref=el.at[:, c2, y2], dst_ref=rl.at[c * ny + y], send_sem=send.at[n], recv_sem=recv.at[n],
                    device_id={'ep': x * CORES + c2, 'sub': y2}, device_id_type=MESH))
    for dx in range(nx):
        for dc in range(CORES):
            if dc or dx:
                x2, c2, n = lax.rem(x + dx, nx), lax.rem(c + dc, CORES), len(copies)
                copies.append(pltpu.make_async_remote_copy(
                    src_ref=er.at[x2, c2], dst_ref=rr.at[x * CORES + c], send_sem=send.at[n], recv_sem=recv.at[n],
                    device_id={'ep': x2 * CORES + c2, 'sub': y}, device_id_type=MESH))
    local = [pltpu.make_async_copy(el.at[:, c, y], rl.at[c * ny + y], own.at[0]),
             pltpu.make_async_copy(er.at[x, c], rr.at[x * CORES + c], own.at[1])]
    return copies, local


def greet(peers):
    barrier = pltpu.get_barrier_semaphore()
    for ep, sub in peers:
        pl.semaphore_signal(barrier, inc=1, device_id={'ep': ep, 'sub': sub}, device_id_type=MESH)
    pl.semaphore_wait(barrier, len(peers))


def greet_exchange(nx, ny):
    x, c, y = place()
    peers = [(x * CORES + lax.rem(c + dc, CORES), lax.rem(y + dy, ny)) for dc in range(CORES) for dy in range(ny) if dc or dy]
    peers += [(lax.rem(x + dx, nx) * CORES + lax.rem(c + dc, CORES), y) for dc in range(CORES) for dx in range(1, nx)]
    greet(peers)


def exchange_kernel(el, er, rl, rr, send, recv, own):
    greet_exchange(el.shape[0], el.shape[2])
    copies, local = exchange_copies(el, er, rl, rr, send, recv, own)
    for copy in copies + local:
        copy.start()
    for copy in copies + local:
        copy.wait()


def exchange_ffn_kernel(el, er, slots, rows, w_gate, w_up, w_down, rl, rr, picked, next_l, next_r, send, recv, own):
    greet_exchange(el.shape[0], el.shape[2])
    copies, local = exchange_copies(el, er, rl, rr, send, recv, own)
    for copy in copies + local:
        copy.start()
    exps, srcs, cap, dim = picked.shape
    toks = rows.shape[1]
    ff = w_gate.shape[-1]
    pltpu.emit_pipeline(
        pick_kernel, grid=(srcs,),
        in_specs=[pl.BlockSpec((1, exps, toks), lambda s: (s, 0, 0)), pl.BlockSpec((1, toks, dim), lambda s: (s, 0, 0))],
        out_specs=[pl.BlockSpec((exps, 1, cap, dim), lambda s: (0, s, 0, 0))],
    )(slots, rows, picked)
    step = 8
    half = dim // 2
    pltpu.emit_pipeline(
        ffn_kernel, grid=(exps, srcs // step),
        in_specs=[
            pl.BlockSpec((1, step, cap, dim), lambda e, s: (e, s, 0, 0)),
            pl.BlockSpec((1, dim, ff), lambda e, s: (e, 0, 0)),
            pl.BlockSpec((1, dim, ff), lambda e, s: (e, 0, 0)),
            pl.BlockSpec((1, ff, dim), lambda e, s: (e, 0, 0)),
        ],
        out_specs=[pl.BlockSpec((step, 1, cap, half), lambda e, s: (s, e, 0, 0))] * 2,
    )(picked, w_gate, w_up, w_down, next_l, next_r)
    for copy in copies + local:
        copy.wait()


ANY = pl.BlockSpec(memory_space=pl.ANY)


def exchange(el, er, collective_id, expert_work=None):
    nx, _, ny, rows, width = el.shape
    shapes = [jax.ShapeDtypeStruct((CORES * ny, nx, rows, width), BF16), jax.ShapeDtypeStruct((nx * CORES, ny, rows, width), BF16)]
    args = [el, er]
    kernel = exchange_kernel
    if expert_work is not None:
        slots, gathered, w_gate, w_up, w_down, cap = expert_work
        srcs, exps, _ = slots.shape
        dim = gathered.shape[-1]
        args += [slots, gathered, w_gate, w_up, w_down]
        shapes += [jax.ShapeDtypeStruct((exps, srcs, cap, dim), BF16)] + [jax.ShapeDtypeStruct((srcs, exps, cap, dim // 2), BF16)] * 2
        kernel = exchange_ffn_kernel
    n = CORES * (nx + ny) - 2
    return pl.pallas_call(
        kernel,
        out_shape=shapes,
        in_specs=[ANY] * len(args),
        out_specs=[ANY] * len(shapes),
        scratch_shapes=[pltpu.SemaphoreType.DMA((n,)), pltpu.SemaphoreType.DMA((n,)), pltpu.SemaphoreType.DMA((2,))],
        compiler_params=pltpu.CompilerParams(collective_id=collective_id, has_side_effects=True, vmem_limit_bytes=VMEM_MAX),
        cost_estimate=pl.CostEstimate(flops=10 ** 11, bytes_accessed=10 ** 8, transcendentals=0),
        name="exchange_rows" if expert_work is None else "exchange_rows_experts",
    )(*args)


def combine_kernel(rl, rr, slot_l, gate_l, slot_r, gate_r, cl, cr, buf_l, buf_r, acc_l, acc_r, load, send_l, send_r, recv_l, recv_r, own):
    nx, ny = rl.shape[1], rr.shape[1]
    x, c, y = place()
    cap_rows = rl.shape[2]

    def load_l(i):
        return pltpu.make_async_copy(rl.at[:, lax.rem(x + i, nx)], buf_l, load.at[0])

    def load_r(i):
        return pltpu.make_async_copy(rr.at[:, lax.rem(y + i, ny)], buf_r, load.at[1])

    def send_left(i):
        x2 = lax.rem(x + i, nx)
        return pltpu.make_async_remote_copy(src_ref=acc_l.at[i], dst_ref=cl.at[x], send_sem=send_l.at[i], recv_sem=recv_l.at[i], device_id={'ep': x2 * CORES + c, 'sub': y}, device_id_type=MESH)

    def send_right(i):
        y2 = lax.rem(y + i, ny)
        return pltpu.make_async_remote_copy(src_ref=acc_r.at[i], dst_ref=cr.at[y], send_sem=send_r.at[i], recv_sem=recv_r.at[i], device_id={'ep': x * CORES + c, 'sub': y2}, device_id_type=MESH)

    def weigh(buf, slot_ref, gate_ref, src, acc, i):
        exps, toks = slot_ref.shape[1:]
        cap = buf.shape[0] * cap_rows // exps
        want = lax.broadcasted_iota(jnp.int32, (cap, toks), 0)
        slots = slot_ref[src]
        hits = [want == slots[e:e + 1, :] for e in range(exps)]
        sels = []
        for part in split3(gate_ref[src]):
            wide = part.astype(F32)
            sels.append(jnp.concatenate([jnp.where(hits[e], wide[e:e + 1, :], 0.0).astype(BF16) for e in range(exps)], axis=0))
        width = acc.shape[-1]
        chunk = 256
        for lo in range(0, width, chunk):
            rows = buf[:, :, lo:lo + chunk].reshape(-1, chunk)
            hi, mid, low = (lax.dot_general(sel, rows, (((0,), (0,)), ((), ())), preferred_element_type=F32) for sel in sels)
            acc[i, :, lo:lo + chunk] = hi + (mid + low)

    load_l(1).start()
    greet([(lax.rem(x + i, nx) * CORES + c, y) for i in range(1, nx)] + [(x * CORES + c, lax.rem(y + i, ny)) for i in range(1, ny)])

    def body(n, carry):
        i = lax.rem(n, nx)
        load_r(n).start()
        load_l(n).wait()
        weigh(buf_l, slot_l, gate_l, lax.rem(x + n, nx), acc_l, i)

        @pl.when(n < nx)
        def _():
            send_left(i).start()
            load_l(n + 1).start()

        load_r(n).wait()
        weigh(buf_r, slot_r, gate_r, lax.rem(y + n, ny), acc_r, i)

        @pl.when(n < nx)
        def _():
            send_right(i).start()

        return carry

    lax.fori_loop(1, nx + 1, body, 0)
    mine = [pltpu.make_async_copy(acc_l.at[0], cl.at[x], own.at[0]), pltpu.make_async_copy(acc_r.at[0], cr.at[y], own.at[1])]
    for copy in mine:
        copy.start()
    for i in range(1, nx):
        send_left(i).wait()
        send_right(i).wait()
    for copy in mine:
        copy.wait()


def combine(rl, rr, left, right, collective_id):
    nx, ny = rl.shape[1], rr.shape[1]
    rows, width = rl.shape[2:]
    toks = left[0].shape[-1]
    vmem = pl.BlockSpec(memory_space=pltpu.VMEM)
    dma = lambda n: pltpu.SemaphoreType.DMA((n,))
    return pl.pallas_call(
        combine_kernel,
        out_shape=[jax.ShapeDtypeStruct((n, toks, width), F32) for n in (nx, ny)],
        in_specs=[ANY, ANY, vmem, vmem, vmem, vmem],
        out_specs=[ANY, ANY],
        scratch_shapes=[
            pltpu.VMEM((rl.shape[0], rows, width), BF16), pltpu.VMEM((rr.shape[0], rows, width), BF16),
            pltpu.VMEM((nx, toks, width), F32), pltpu.VMEM((ny, toks, width), F32),
            dma(2), dma(nx), dma(ny), dma(nx), dma(ny), dma(2),
        ],
        compiler_params=pltpu.CompilerParams(collective_id=collective_id, has_side_effects=True, vmem_limit_bytes=VMEM_MAX),
        cost_estimate=pl.CostEstimate(flops=10 ** 11, bytes_accessed=10 ** 8, transcendentals=0),
        name="combine_rows",
    )(rl, rr, *left, *right)


def solution(mesh):
    ep_size = mesh.shape['ep']
    sub_size = mesh.shape['sub']
    axes = ('ep', 'sub')
    tok_spec = P(('dp', 'ep', 'sub'), None, None)
    route_spec = P(None, ('dp', 'ep', 'sub'), None)
    exp_spec = P(('ep', 'sub'), None, None)

    def device_body(input_a, input_b, route_idx, route_gate, attn_norm, w_query, w_key, w_value, w_out, moe_norm, w_gate, w_up, w_down):
        exp_local = w_gate.shape[0]
        num_dev = ep_size * sub_size
        num_exp = exp_local * num_dev
        tok_count, top_k = route_idx.shape[1:]
        model_dim = input_a.shape[-1]
        cap = 3 * top_k * tok_count // (2 * num_exp)
        first_exp = lax.axis_index(axes) * exp_local

        nx, ny = ep_size // CORES, sub_size
        x, c, y = place()
        ids_all = lax.all_gather(jnp.swapaxes(route_idx, 1, 2), axes, axis=0)
        gates_all = lax.all_gather(jnp.swapaxes(route_gate, 1, 2), axes, axis=0)

        weights = (attn_norm, w_query, w_key, w_value, w_out)
        hiddens, gathered = [], []
        after = None
        for tokens, ranges in ((input_a, 2), (input_b, 1)):
            rows_all = tokens.reshape(tok_count, model_dim)
            step = tok_count // ranges
            ks, vs, parts, blocks = [], [], [], []
            for r in range(ranges):
                rows = rows_all[r * step:(r + 1) * step]
                if after is not None:
                    rows, after = lax.optimization_barrier((rows, after))
                hidden, ks, vs = attention_rows(rows, ks, vs, *weights)
                after = rms_norm(hidden, moe_norm)
                blocks.append(lax.all_gather(after, axes, axis=0))
                parts.append(hidden)
            hiddens.append(jnp.concatenate(parts, axis=0) if ranges > 1 else parts[0])
            gathered.append(blocks)

        def grid_of(t):
            return t.reshape(nx, CORES, ny, exp_local * cap, model_dim // 2)

        def selects(mb):
            ids = ids_all.reshape(nx, CORES, ny, 2, top_k, tok_count)
            gates = gates_all.reshape(nx, CORES, ny, 2, top_k, tok_count)
            in_column = x * (CORES * ny * exp_local) + jnp.arange(CORES * ny * exp_local, dtype=jnp.int32)
            in_row = (jnp.arange(ep_size, dtype=jnp.int32)[:, None] * (ny * exp_local) + y * exp_local + jnp.arange(exp_local, dtype=jnp.int32)[None, :]).reshape(-1)
            left = sources_select(ids[:, c, y, mb], gates[:, c, y, mb], in_column)
            right = sources_select(ids[x, c, :, mb], gates[x, c, :, mb], in_row)
            return left, right

        slots = [slots_here(ids_all[:, mb], first_exp, exp_local) for mb in range(2)]
        first = expert_ffn(pick_rows(slots[0], gathered[0], cap), w_gate, w_up, w_down, 2)
        rows_l, rows_r, _, *second = exchange(*map(grid_of, first), 0, (slots[1], gathered[1][0], w_gate, w_up, w_down, cap))
        sums = [combine(rows_l, rows_r, *selects(0), 1)]
        sums.append(combine(*exchange(*map(grid_of, second), 2), *selects(1), 3))
        outs = []
        for hidden, (cl, cr), tokens in zip(hiddens, sums, (input_a, input_b)):
            moe_sum = jnp.concatenate([jnp.sum(cl, axis=0), jnp.sum(cr, axis=0)], axis=1)
            outs.append((hidden.astype(F32) + moe_sum).astype(BF16).reshape(tokens.shape))
        return outs[0], outs[1]

    return jax.shard_map(device_body, mesh=mesh, in_specs=(tok_spec, tok_spec, route_spec, route_spec, P(), P(), P(), P(), P(), P(), exp_spec, exp_spec, exp_spec), out_specs=(tok_spec, tok_spec), check_vma=False)
```

```python
import functools

import jax
import jax.numpy as jnp
from jax import lax
from jax.experimental import pallas as pl
from jax.experimental.pallas import tpu as pltpu
from jax.sharding import PartitionSpec as P

NORM_EPS = 1e-6
VMEM_MAX = 60 * 1024 * 1024
F32 = jnp.float32
BF16 = jnp.bfloat16
MESH = pl.DeviceIdType.MESH
CORES = 2


def rms_norm(values, norm_gain):
    acc_f32 = values.astype(F32)
    inv_rms = lax.rsqrt(jnp.mean(acc_f32 * acc_f32, axis=-1, keepdims=True) + NORM_EPS)
    return (acc_f32 * inv_rms * norm_gain).astype(BF16)


def attn_kernel(scale, first, q_ref, *refs):
    k_refs, v_refs, o_ref = refs[:first + 1], refs[first + 1:2 * first + 2], refs[-1]
    heads, q_len, head_dim = q_ref.shape
    parts = 2 if first == 0 and q_len >= 512 else 1
    rows_per = q_len // parts
    for h in range(heads):
        for part in range(parts):
            q = q_ref[h, part * rows_per:(part + 1) * rows_per, :]
            spans = [(k_refs[i], v_refs[i], 0, k_refs[i].shape[1], False) for i in range(first)]
            if part:
                spans.append((k_refs[first], v_refs[first], 0, part * rows_per, False))
            spans.append((k_refs[first], v_refs[first], part * rows_per, (part + 1) * rows_per, True))
            scores = []
            for k_ref, _, lo, hi, diagonal in spans:
                s = lax.dot_general(q, k_ref[h, lo:hi, :], (((1,), (1,)), ((), ())), preferred_element_type=F32) * scale
                if diagonal:
                    rows = lax.broadcasted_iota(jnp.int32, s.shape, 0)
                    cols = lax.broadcasted_iota(jnp.int32, s.shape, 1)
                    s = jnp.where(rows >= cols, s, -jnp.inf)
                scores.append(s)
            top = functools.reduce(jnp.maximum, [jnp.max(s, axis=-1, keepdims=True) for s in scores])
            probs = [jnp.exp(s - top) for s in scores]
            inv = 1.0 / functools.reduce(jnp.add, [jnp.sum(p, axis=-1, keepdims=True) for p in probs])
            o = None
            for p, (_, v_ref, lo, hi, _) in zip(probs, spans):
                term = jnp.dot((p * inv).astype(BF16), v_ref[h, lo:hi, :], preferred_element_type=F32)
                o = term if o is None else o + term
            o_ref[part * rows_per:(part + 1) * rows_per, h * head_dim:(h + 1) * head_dim] = o.astype(BF16)


def attention_core(q, ks, vs):
    heads, q_len, head_dim = q.shape
    step = 4
    spec = lambda t: pl.BlockSpec((step, t.shape[1], head_dim), lambda i: (i, 0, 0))
    keys = sum(k.shape[1] for k in ks)
    return pl.pallas_call(
        functools.partial(attn_kernel, head_dim ** -0.5, len(ks) - 1),
        grid=(heads // step,),
        out_shape=jax.ShapeDtypeStruct((q_len, heads * head_dim), BF16),
        in_specs=[spec(t) for t in (q, *ks, *vs)],
        out_specs=pl.BlockSpec((q_len, step * head_dim), lambda i: (0, i)),
        cost_estimate=pl.CostEstimate(flops=4 * heads * q_len * keys * head_dim, bytes_accessed=4 * heads * (q_len + keys) * head_dim, transcendentals=heads * q_len * keys),
        name="attention_core",
    )(q, *ks, *vs)


def attention_rows(rows, ks, vs, attn_norm, w_query, w_key, w_value, w_out):
    normed = rms_norm(rows, attn_norm)
    q, k, v = (jnp.einsum('sd,dhc->hsc', normed, w, preferred_element_type=F32).astype(BF16) for w in (w_query, w_key, w_value))
    ks, vs = ks + [k], vs + [v]
    context = attention_core(q, ks, vs)
    proj_out = jnp.dot(context, w_out.reshape(-1, w_out.shape[-1]), preferred_element_type=F32)
    return (rows.astype(F32) + proj_out).astype(BF16), ks, vs


def pick_kernel(slot_ref, *refs):
    row_refs, out_ref = refs[:-1], refs[-1]
    exp_local, _, cap, dim = out_ref.shape
    total = None
    lo = 0
    for rows_ref in row_refs:
        toks = rows_ref.shape[1]
        want = lax.broadcasted_iota(jnp.int32, (cap, toks), 0)
        sel = jnp.concatenate([(want == slot_ref[0, e:e + 1, lo:lo + toks]).astype(F32) for e in range(exp_local)], axis=0).astype(BF16)
        term = jnp.dot(sel, rows_ref[0], preferred_element_type=F32)
        total = term if total is None else total + term
        lo += toks
    out_ref[:, 0] = total.astype(BF16).reshape(exp_local, cap, dim)


def pick_rows(slots, ranges, cap):
    srcs, exps, toks = slots.shape
    dim = ranges[0].shape[-1]
    return pl.pallas_call(
        pick_kernel,
        grid=(srcs,),
        out_shape=jax.ShapeDtypeStruct((exps, srcs, cap, dim), BF16),
        in_specs=[pl.BlockSpec((1, exps, toks), lambda s: (s, 0, 0))] + [pl.BlockSpec((1, r.shape[1], dim), lambda s: (s, 0, 0)) for r in ranges],
        out_specs=pl.BlockSpec((exps, 1, cap, dim), lambda s: (0, s, 0, 0)),
        cost_estimate=pl.CostEstimate(flops=2 * srcs * exps * cap * toks * dim, bytes_accessed=2 * srcs * (toks + exps * cap) * dim, transcendentals=0),
        name="pick_rows",
    )(slots, *ranges)


def ffn_kernel(x_ref, wg_ref, wu_ref, wd_ref, *o_refs):
    _, srcs, cap, dim = x_ref.shape
    x = x_ref[0].reshape(srcs * cap, dim)
    gate_h = jnp.dot(x, wg_ref[0], preferred_element_type=F32)
    up_h = jnp.dot(x, wu_ref[0], preferred_element_type=F32)
    act = (jax.nn.silu(gate_h) * up_h).astype(BF16)
    y = jnp.dot(act, wd_ref[0], preferred_element_type=F32).astype(BF16)
    lo = 0
    for o_ref in o_refs:
        width = o_ref.shape[-1]
        o_ref[:, 0] = y[:, lo:lo + width].reshape(srcs, cap, width)
        lo += width


def expert_ffn(x, w_gate, w_up, w_down, pieces):
    exps, srcs, cap, dim = x.shape
    ff = w_gate.shape[-1]
    step = 8
    width = dim // pieces
    return pl.pallas_call(
        ffn_kernel,
        grid=(exps, srcs // step),
        out_shape=[jax.ShapeDtypeStruct((srcs, exps, cap, width), BF16)] * pieces,
        in_specs=[
            pl.BlockSpec((1, step, cap, dim), lambda e, s: (e, s, 0, 0)),
            pl.BlockSpec((1, dim, ff), lambda e, s: (e, 0, 0)),
            pl.BlockSpec((1, dim, ff), lambda e, s: (e, 0, 0)),
            pl.BlockSpec((1, ff, dim), lambda e, s: (e, 0, 0)),
        ],
        out_specs=[pl.BlockSpec((step, 1, cap, width), lambda e, s: (s, e, 0, 0))] * pieces,
        cost_estimate=pl.CostEstimate(flops=6 * exps * srcs * cap * dim * ff, bytes_accessed=4 * exps * srcs * cap * dim + 6 * exps * dim * ff, transcendentals=exps * srcs * cap * ff),
        compiler_params=pltpu.CompilerParams(vmem_limit_bytes=VMEM_MAX),
        name="expert_ffn",
    )(x, w_gate, w_up, w_down)


def split3(x):
    hi = x.astype(BF16)
    rest = x - hi.astype(F32)
    mid = rest.astype(BF16)
    low = (rest - mid.astype(F32)).astype(BF16)
    return hi, mid, low


def ranks_of(mask, axis):
    toks = mask.shape[axis]
    row = lax.broadcasted_iota(jnp.int32, (toks, toks), 0)
    col = lax.broadcasted_iota(jnp.int32, (toks, toks), 1)
    if axis == mask.ndim - 1:
        tri = (row < col).astype(BF16)
        return jnp.dot(mask.astype(BF16), tri, preferred_element_type=F32).astype(jnp.int32)
    tri = (row > col).astype(BF16)
    return jnp.dot(tri, mask.astype(BF16), preferred_element_type=F32).astype(jnp.int32)


def slots_here(ids_all, first_exp, exp_local):
    mine = first_exp + jnp.arange(exp_local, dtype=jnp.int32)
    mask = jnp.any(ids_all[:, None] == mine[None, :, None, None], axis=2)
    srcs, exps, toks = mask.shape
    rank = ranks_of(mask.reshape(srcs * exps, toks), 1).reshape(srcs, exps, toks)
    return jnp.where(mask, rank, -1)


def sources_select(ids, gates, experts):
    hit = ids[:, None] == experts[None, :, None, None]
    mask = jnp.any(hit, axis=2)
    gate = jnp.sum(jnp.where(hit, gates[:, None], 0.0), axis=2)
    srcs, exps, toks = mask.shape
    rank = ranks_of(mask.reshape(srcs * exps, toks), 1).reshape(srcs, exps, toks)
    return jnp.where(mask, rank, -1), gate


def place():
    ep = lax.axis_index('ep')
    return lax.div(ep, CORES), lax.rem(ep, CORES), lax.axis_index('sub')


def exchange_copies(el, er, rl, rr, send, recv, own):
    nx, _, ny = el.shape[:3]
    x, c, y = place()
    copies = []
    for dc in range(CORES):
        for dy in range(ny):
            if dc or dy:
                c2, y2, n = lax.rem(c + dc, CORES), lax.rem(y + dy, ny), len(copies)
                copies.append(pltpu.make_async_remote_copy(
                    src_ref=el.at[:, c2, y2], dst_ref=rl.at[c * ny + y], send_sem=send.at[n], recv_sem=recv.at[n],
                    device_id={'ep': x * CORES + c2, 'sub': y2}, device_id_type=MESH))
    for dx in range(nx):
        for dc in range(CORES):
            if dc or dx:
                x2, c2, n = lax.rem(x + dx, nx), lax.rem(c + dc, CORES), len(copies)
                copies.append(pltpu.make_async_remote_copy(
                    src_ref=er.at[x2, c2], dst_ref=rr.at[x * CORES + c], send_sem=send.at[n], recv_sem=recv.at[n],
                    device_id={'ep': x2 * CORES + c2, 'sub': y}, device_id_type=MESH))
    local = [pltpu.make_async_copy(el.at[:, c, y], rl.at[c * ny + y], own.at[0]),
             pltpu.make_async_copy(er.at[x, c], rr.at[x * CORES + c], own.at[1])]
    return copies, local


def greet(peers):
    barrier = pltpu.get_barrier_semaphore()
    for ep, sub in peers:
        pl.semaphore_signal(barrier, inc=1, device_id={'ep': ep, 'sub': sub}, device_id_type=MESH)
    pl.semaphore_wait(barrier, len(peers))


def greet_exchange(nx, ny):
    x, c, y = place()
    peers = [(x * CORES + lax.rem(c + dc, CORES), lax.rem(y + dy, ny)) for dc in range(CORES) for dy in range(ny) if dc or dy]
    peers += [(lax.rem(x + dx, nx) * CORES + lax.rem(c + dc, CORES), y) for dc in range(CORES) for dx in range(1, nx)]
    greet(peers)


def exchange_kernel(el, er, rl, rr, send, recv, own):
    greet_exchange(el.shape[0], el.shape[2])
    copies, local = exchange_copies(el, er, rl, rr, send, recv, own)
    for copy in copies + local:
        copy.start()
    for copy in copies + local:
        copy.wait()


def exchange_ffn_kernel(el, er, slots, rows, w_gate, w_up, w_down, rl, rr, picked, next_l, next_r, send, recv, own):
    greet_exchange(el.shape[0], el.shape[2])
    copies, local = exchange_copies(el, er, rl, rr, send, recv, own)
    for copy in copies + local:
        copy.start()
    exps, srcs, cap, dim = picked.shape
    toks = rows.shape[1]
    ff = w_gate.shape[-1]
    pltpu.emit_pipeline(
        pick_kernel, grid=(srcs,),
        in_specs=[pl.BlockSpec((1, exps, toks), lambda s: (s, 0, 0)), pl.BlockSpec((1, toks, dim), lambda s: (s, 0, 0))],
        out_specs=[pl.BlockSpec((exps, 1, cap, dim), lambda s: (0, s, 0, 0))],
    )(slots, rows, picked)
    step = 8
    half = dim // 2
    pltpu.emit_pipeline(
        ffn_kernel, grid=(exps, srcs // step),
        in_specs=[
            pl.BlockSpec((1, step, cap, dim), lambda e, s: (e, s, 0, 0)),
            pl.BlockSpec((1, dim, ff), lambda e, s: (e, 0, 0)),
            pl.BlockSpec((1, dim, ff), lambda e, s: (e, 0, 0)),
            pl.BlockSpec((1, ff, dim), lambda e, s: (e, 0, 0)),
        ],
        out_specs=[pl.BlockSpec((step, 1, cap, half), lambda e, s: (s, e, 0, 0))] * 2,
    )(picked, w_gate, w_up, w_down, next_l, next_r)
    for copy in copies + local:
        copy.wait()


ANY = pl.BlockSpec(memory_space=pl.ANY)


def exchange(el, er, collective_id, expert_work=None):
    nx, _, ny, rows, width = el.shape
    shapes = [jax.ShapeDtypeStruct((CORES * ny, nx, rows, width), BF16), jax.ShapeDtypeStruct((nx * CORES, ny, rows, width), BF16)]
    args = [el, er]
    kernel = exchange_kernel
    if expert_work is not None:
        slots, gathered, w_gate, w_up, w_down, cap = expert_work
        srcs, exps, _ = slots.shape
        dim = gathered.shape[-1]
        args += [slots, gathered, w_gate, w_up, w_down]
        shapes += [jax.ShapeDtypeStruct((exps, srcs, cap, dim), BF16)] + [jax.ShapeDtypeStruct((srcs, exps, cap, dim // 2), BF16)] * 2
        kernel = exchange_ffn_kernel
    n = CORES * (nx + ny) - 2
    return pl.pallas_call(
        kernel,
        out_shape=shapes,
        in_specs=[ANY] * len(args),
        out_specs=[ANY] * len(shapes),
        scratch_shapes=[pltpu.SemaphoreType.DMA((n,)), pltpu.SemaphoreType.DMA((n,)), pltpu.SemaphoreType.DMA((2,))],
        compiler_params=pltpu.CompilerParams(collective_id=collective_id, has_side_effects=True, vmem_limit_bytes=VMEM_MAX),
        cost_estimate=pl.CostEstimate(flops=10 ** 11, bytes_accessed=10 ** 8, transcendentals=0),
        name="exchange_rows" if expert_work is None else "exchange_rows_experts",
    )(*args)


def combine_kernel(rl, rr, slot_l, gate_l, slot_r, gate_r, hidden, out, buf_l, buf_r, acc_l, acc_r, cl, cr, load, send_l, send_r, recv_l, recv_r):
    nx, ny = rl.shape[1], rr.shape[1]
    x, c, y = place()
    cap_rows = rl.shape[2]

    def load_l(i):
        return pltpu.make_async_copy(rl.at[:, lax.rem(x + i, nx)], buf_l, load.at[0])

    def load_r(i):
        return pltpu.make_async_copy(rr.at[:, lax.rem(y + i, ny)], buf_r, load.at[1])

    def send_left(i):
        x2 = lax.rem(x + i, nx)
        return pltpu.make_async_remote_copy(src_ref=acc_l.at[i], dst_ref=cl.at[i], send_sem=send_l.at[i], recv_sem=recv_l.at[i], device_id={'ep': x2 * CORES + c, 'sub': y}, device_id_type=MESH)

    def send_right(i):
        y2 = lax.rem(y + i, ny)
        return pltpu.make_async_remote_copy(src_ref=acc_r.at[i], dst_ref=cr.at[i], send_sem=send_r.at[i], recv_sem=recv_r.at[i], device_id={'ep': x * CORES + c, 'sub': y2}, device_id_type=MESH)

    def weigh(buf, slot_ref, gate_ref, src, acc, i):
        exps, toks = slot_ref.shape[1:]
        cap = buf.shape[0] * cap_rows // exps
        want = lax.broadcasted_iota(jnp.int32, (cap, toks), 0)
        slots = slot_ref[src]
        hits = [want == slots[e:e + 1, :] for e in range(exps)]
        sels = []
        for part in split3(gate_ref[src]):
            wide = part.astype(F32)
            sels.append(jnp.concatenate([jnp.where(hits[e], wide[e:e + 1, :], 0.0).astype(BF16) for e in range(exps)], axis=0))
        width = acc.shape[-1]
        chunk = 256
        for lo in range(0, width, chunk):
            rows = buf[:, :, lo:lo + chunk].reshape(-1, chunk)
            hi, mid, low = (lax.dot_general(sel, rows, (((0,), (0,)), ((), ())), preferred_element_type=F32) for sel in sels)
            acc[i, :, lo:lo + chunk] = hi + (mid + low)

    def turn(n, size):
        return lax.rem(size // 2 + 1 + (size - 1) * n, size)

    load_l(turn(1, nx)).start()
    greet([(lax.rem(x + i, nx) * CORES + c, y) for i in range(1, nx)] + [(x * CORES + c, lax.rem(y + i, ny)) for i in range(1, ny)])

    def body(n, carry):
        i, j = turn(n, nx), turn(n, ny)
        load_r(j).start()
        load_l(i).wait()
        weigh(buf_l, slot_l, gate_l, lax.rem(x + i, nx), acc_l, i)

        @pl.when(i > 0)
        def _():
            send_left(i).start()

        @pl.when(n < nx)
        def _():
            load_l(turn(n + 1, nx)).start()

        load_r(j).wait()
        weigh(buf_r, slot_r, gate_r, lax.rem(y + j, ny), acc_r, j)

        @pl.when(j > 0)
        def _():
            send_right(j).start()

        return carry

    lax.fori_loop(1, nx + 1, body, 0)
    for i in range(1, nx):
        send_left(i).wait()
        send_right(i).wait()
    toks, width = acc_l.shape[1:]
    step = min(64, toks)

    def finish(n, carry):
        at = pl.ds(pl.multiple_of(n * step, step), step)
        for side, (acc, got) in enumerate(((acc_l, cl), (acc_r, cr))):
            total = acc[0, at, :]
            for i in range(1, got.shape[0]):
                total = total + got[i, at, :]
            cols = slice(side * width, (side + 1) * width)
            out[at, cols] = (hidden[at, cols].astype(F32) + total).astype(BF16)
        return carry

    lax.fori_loop(0, toks // step, finish, 0)


def combine(rl, rr, left, right, hidden, collective_id):
    nx, ny = rl.shape[1], rr.shape[1]
    rows, width = rl.shape[2:]
    toks = left[0].shape[-1]
    vmem = pl.BlockSpec(memory_space=pltpu.VMEM)
    dma = lambda n: pltpu.SemaphoreType.DMA((n,))
    return pl.pallas_call(
        combine_kernel,
        out_shape=jax.ShapeDtypeStruct(hidden.shape, BF16),
        in_specs=[ANY, ANY] + [vmem] * 5,
        out_specs=vmem,
        scratch_shapes=[
            pltpu.VMEM((rl.shape[0], rows, width), BF16), pltpu.VMEM((rr.shape[0], rows, width), BF16),
            pltpu.VMEM((nx, toks, width), F32), pltpu.VMEM((ny, toks, width), F32),
            pltpu.VMEM((nx, toks, width), F32), pltpu.VMEM((ny, toks, width), F32),
            dma(2), dma(nx), dma(ny), dma(nx), dma(ny),
        ],
        compiler_params=pltpu.CompilerParams(collective_id=collective_id, has_side_effects=True, vmem_limit_bytes=VMEM_MAX),
        cost_estimate=pl.CostEstimate(flops=10 ** 11, bytes_accessed=10 ** 8, transcendentals=0),
        name="combine_rows",
    )(rl, rr, *left, *right, hidden)


def solution(mesh):
    ep_size = mesh.shape['ep']
    sub_size = mesh.shape['sub']
    axes = ('ep', 'sub')
    tok_spec = P(('dp', 'ep', 'sub'), None, None)
    route_spec = P(None, ('dp', 'ep', 'sub'), None)
    exp_spec = P(('ep', 'sub'), None, None)

    def device_body(input_a, input_b, route_idx, route_gate, attn_norm, w_query, w_key, w_value, w_out, moe_norm, w_gate, w_up, w_down):
        exp_local = w_gate.shape[0]
        num_dev = ep_size * sub_size
        num_exp = exp_local * num_dev
        tok_count, top_k = route_idx.shape[1:]
        model_dim = input_a.shape[-1]
        cap = 3 * top_k * tok_count // (2 * num_exp)
        first_exp = lax.axis_index(axes) * exp_local

        nx, ny = ep_size // CORES, sub_size
        x, c, y = place()
        ids_all = lax.all_gather(jnp.swapaxes(route_idx, 1, 2), axes, axis=0)
        gates_all = lax.all_gather(jnp.swapaxes(route_gate, 1, 2), axes, axis=0)

        weights = (attn_norm, w_query, w_key, w_value, w_out)
        hiddens, gathered = [], []
        after = None
        for tokens, ranges in ((input_a, 1), (input_b, 1)):
            rows_all = tokens.reshape(tok_count, model_dim)
            step = tok_count // ranges
            ks, vs, parts, blocks = [], [], [], []
            for r in range(ranges):
                rows = rows_all[r * step:(r + 1) * step]
                if after is not None:
                    rows, after = lax.optimization_barrier((rows, after))
                hidden, ks, vs = attention_rows(rows, ks, vs, *weights)
                after = rms_norm(hidden, moe_norm)
                blocks.append(lax.all_gather(after, axes, axis=0))
                parts.append(hidden)
            hiddens.append(jnp.concatenate(parts, axis=0) if ranges > 1 else parts[0])
            gathered.append(blocks)

        def grid_of(t):
            return t.reshape(nx, CORES, ny, exp_local * cap, model_dim // 2)

        def selects(mb):
            ids = ids_all.reshape(nx, CORES, ny, 2, top_k, tok_count)
            gates = gates_all.reshape(nx, CORES, ny, 2, top_k, tok_count)
            in_column = x * (CORES * ny * exp_local) + jnp.arange(CORES * ny * exp_local, dtype=jnp.int32)
            in_row = (jnp.arange(ep_size, dtype=jnp.int32)[:, None] * (ny * exp_local) + y * exp_local + jnp.arange(exp_local, dtype=jnp.int32)[None, :]).reshape(-1)
            left = sources_select(ids[:, c, y, mb], gates[:, c, y, mb], in_column)
            right = sources_select(ids[x, c, :, mb], gates[x, c, :, mb], in_row)
            return left, right

        slots = [slots_here(ids_all[:, mb], first_exp, exp_local) for mb in range(2)]
        first = expert_ffn(pick_rows(slots[0], gathered[0], cap), w_gate, w_up, w_down, 2)
        rows_l, rows_r, _, *second = exchange(*map(grid_of, first), 0, (slots[1], gathered[1][0], w_gate, w_up, w_down, cap))
        outs = [combine(rows_l, rows_r, *selects(0), hiddens[0], 1)]
        outs.append(combine(*exchange(*map(grid_of, second), 2), *selects(1), hiddens[1], 3))
        outs = [out.reshape(tokens.shape) for out, tokens in zip(outs, (input_a, input_b))]
        return outs[0], outs[1]

    return jax.shard_map(device_body, mesh=mesh, in_specs=(tok_spec, tok_spec, route_spec, route_spec, P(), P(), P(), P(), P(), P(), exp_spec, exp_spec, exp_spec), out_specs=(tok_spec, tok_spec), check_vma=False)
```
